32 devices in a mesh: branch: 2 (over x), seq: 16 (over z, y, core).
Axes of the slice: x: 2, y: 2, z: 4, core: 2. Of those that a mesh axis runs over, the one named last changes fastest.
Arguments:
- queries: bfloat16 [8192, 2048], P(('branch', 'seq')), parts along dimension 0, may hold values from -8 to 8
- keys: bfloat16 [8192, 2048], P(('branch', 'seq')), parts along dimension 0, may hold values from -8 to 8
- values: bfloat16 [8192, 2048], P(('branch', 'seq')), parts along dimension 0, may hold values from -6 to 6
- out_grad: bfloat16 [8192, 2048], P(('branch', 'seq')), parts along dimension 0, may hold values from -6 to 6
- segments: int32 [8192], P(('branch', 'seq')), parts along dimension 0, may hold values from 0 to 7, never falling along the last dimension, each value on 1 to 768 neighbouring positions
Outputs:
- attended: bfloat16 [8192, 2048], P(('branch', 'seq')), parts along dimension 0
- query_grad: bfloat16 [8192, 2048], P(('branch', 'seq')), parts along dimension 0
- key_grad: bfloat16 [8192, 2048], P(('branch', 'seq')), parts along dimension 0
- value_grad: bfloat16 [8192, 2048], P(('branch', 'seq')), parts along dimension 0
The draws below stay inside these ranges and needn't reach their ends.
There are 2 independent parts, one for each index of `branch`. The reference program is written for one: setup_inputs(seed, part) draws one part's arguments, and reference() takes and returns one part's arrays. A program takes and returns all parts, laid end to end along the dimension named above; each array names one. Nothing has to cross between parts.
Inputs may be any that keep to these rules, and one draw needn't show every extreme that they name: `segments`: never falling along the sequence; each document has 1 to 768 tokens, and one has exactly 768.
All inputs are finite; a program needn't handle non-finite values.
Results may differ from the reference program's by a relative error of at most 0.017.
Values may be sent and summed in bfloat16 or wider, within the bound.
No kernel may reach another device: no remote copies, remote signals or barrier semaphores. Data moves between devices by JAX's collectives and lax.ppermute only.
A program may use at most 128 MiB of HBM per device.

```python
import math
import jax
import jax.numpy as jnp
import numpy as np
from jax import lax

HEADS = 16
HDIM = 128
TOK_DEV = 256
REACH = 3
DOC_MAX = 768
TOKENS = 4096
DOCS = 8


def draw_queries(key, part):
    noise_key = jax.random.fold_in(key, 11)
    noise = jax.random.truncated_normal(noise_key, -6.0, 6.0, (TOKENS, HEADS * HDIM), jnp.float32)
    return noise.astype(jnp.bfloat16)


def draw_keys(key, part):
    noise_key = jax.random.fold_in(key, 13)
    noise = jax.random.truncated_normal(noise_key, -6.0, 6.0, (TOKENS, HEADS * HDIM), jnp.float32)
    return noise.astype(jnp.bfloat16)


def steps_of(rng, extent, cuts, smallest, high):
    def one(dim, blocks):
        heights = jax.random.uniform(jax.random.fold_in(jax.random.fold_in(rng, 6), dim), (blocks,), jnp.float32, smallest / len(cuts), high / len(cuts))
        return jnp.repeat(jnp.exp(heights), extent[dim] // blocks).reshape((-1,) + (1,) * (len(extent) - dim - 1))

    factor_of = one(*cuts[0])
    for cut in cuts[1:]:
        factor_of = factor_of * one(*cut)
    return factor_of


def length_profile(amount, total, most, skew):
    weights = [(1 << 20) // math.isqrt(standing ** skew) + 1 for standing in range(2, amount + 1)]
    rest, holding = total - most - (amount - 1), [1] * (amount - 1)
    while rest > 0:
        candidates = [i for i in range(amount - 1) if holding[i] < most]
        mass, budget = sum([weights[i] for i in candidates]), rest
        for i in candidates:
            addition = min(most - holding[i], max(1, budget * weights[i] // mass), rest)
            holding[i] = holding[i] + addition
            rest = rest - addition
    return np.array([most] + holding)


def ragged_sizes(own_key, count, total, reach, slope):
    if count == 2:
        one = jax.random.randint(own_key, (), max(1, total - reach), min(reach, total - 1) + 1)
        return jnp.stack([one, total - one])
    lengths = jnp.asarray(length_profile(count, total, reach, slope), jnp.int32)
    pairs = (count - 1) // 2
    donor, sink = lengths[1:1 + 2 * pairs:2], lengths[2:2 + 2 * pairs:2]
    margin = jnp.minimum(donor - 1, reach - sink)
    moved = jax.random.randint(jax.random.fold_in(own_key, 1), (pairs,), 0, 1 << 20) % (margin + 1)
    lengths = lengths.at[1:1 + 2 * pairs:2].set(donor - moved).at[2:2 + 2 * pairs:2].set(sink + moved)
    return lengths[jax.random.permutation(jax.random.fold_in(own_key, 2), count)]


def bell_draw(stream_key, dims, deviation, most, shards=(), kind=jnp.bfloat16):
    values = jax.random.normal(stream_key, dims, jnp.float32) * deviation
    if len(shards) > 0:
        values = steps_of(stream_key, dims, shards, -0.22, 0.18) * values
    return jnp.clip(values, min=-most, max=most).astype(kind)


def setup_inputs(seed: int = 0, part: int = 0) -> dict:
    arg_keys = jax.random.split(jax.random.key(seed), 6)
    part_keys = jax.random.split(jax.random.fold_in(arg_keys[5], part), 6)
    return {
        "queries": draw_queries(jax.random.fold_in(jax.random.fold_in(arg_keys[5], part), 71), part),
        "keys": draw_keys(jax.random.fold_in(jax.random.fold_in(arg_keys[5], part), 71), part),
        "values": bell_draw(part_keys[2], (TOKENS, HEADS * HDIM), 1.0, 6.0, ((0, 16),)),
        "out_grad": bell_draw(part_keys[3], (TOKENS, HEADS * HDIM), 1.0, 6.0, ((0, 16),)),
        "segments": jnp.searchsorted(jnp.cumsum(ragged_sizes(part_keys[4], DOCS, TOKENS, DOC_MAX, 1)), jnp.arange(TOKENS), side="right").astype(jnp.int32),
    }


def to_half(tensor):
    return lax.optimization_barrier(tensor.astype(jnp.bfloat16)).astype(jnp.float32)

def reference(queries, keys, values, out_grad, segments):
    inv_root = 1.0 / math.sqrt(HDIM)
    pad_rows = REACH * TOK_DEV
    key_width = (REACH + 1) * TOK_DEV
    feature = HEADS * HDIM
    keys_padded = jnp.concatenate([jnp.zeros((pad_rows, feature), keys.dtype), keys], 0)
    values_padded = jnp.concatenate([jnp.zeros((pad_rows, feature), values.dtype), values], 0)
    seg_padded = jnp.concatenate([jnp.full((pad_rows,), -1, jnp.int32), segments.astype(jnp.int32)], 0)

    def one_block(carry, block_index):
        key_acc, value_acc = carry
        start = (block_index * TOK_DEV).astype(jnp.int32)
        query_block = lax.dynamic_slice_in_dim(queries, start, TOK_DEV, 0).reshape(TOK_DEV, HEADS, HDIM).astype(jnp.float32)
        grad_block = lax.dynamic_slice_in_dim(out_grad, start, TOK_DEV, 0).reshape(TOK_DEV, HEADS, HDIM).astype(jnp.float32)
        key_block = lax.dynamic_slice_in_dim(keys_padded, start, key_width, 0).reshape(key_width, HEADS, HDIM).astype(jnp.float32)
        value_block = lax.dynamic_slice_in_dim(values_padded, start, key_width, 0).reshape(key_width, HEADS, HDIM).astype(jnp.float32)
        query_seg = lax.dynamic_slice_in_dim(segments.astype(jnp.int32), start, TOK_DEV, 0)
        key_seg = lax.dynamic_slice_in_dim(seg_padded, start, key_width, 0)
        query_pos = start + jnp.arange(TOK_DEV, dtype=jnp.int32)
        key_pos = start - pad_rows + jnp.arange(key_width, dtype=jnp.int32)
        visible = (key_pos[None, :] <= query_pos[:, None]) & (key_seg[None, :] == query_seg[:, None])
        scores = jnp.einsum('ihd,jhd->hij', query_block, key_block) * inv_root
        scores = jnp.where(visible[None], scores, -jnp.inf)
        row_peak = lax.optimization_barrier(jnp.max(scores, -1, keepdims=True))
        exponent = jnp.exp(scores - row_peak)
        row_total = lax.optimization_barrier(jnp.sum(exponent, -1, keepdims=True))
        weights = to_half(exponent / row_total)
        attended = jnp.einsum('hij,jhd->ihd', weights, value_block).astype(jnp.bfloat16)
        dprob = jnp.einsum('ihd,jhd->hij', grad_block, value_block)
        row_delta = lax.optimization_barrier(jnp.sum(grad_block * attended.astype(jnp.float32), -1)).T
        dscore = to_half(weights * (dprob - row_delta[:, :, None]) * inv_root)
        query_grad = jnp.einsum('hij,jhd->ihd', dscore, key_block).astype(jnp.bfloat16)
        key_part = jnp.einsum('hij,ihd->jhd', dscore, query_block).reshape(key_width, feature)
        value_part = jnp.einsum('hij,ihd->jhd', weights, grad_block).reshape(key_width, feature)
        key_acc = lax.dynamic_update_slice_in_dim(key_acc, lax.dynamic_slice_in_dim(key_acc, start, key_width, 0) + key_part, start, 0)
        value_acc = lax.dynamic_update_slice_in_dim(value_acc, lax.dynamic_slice_in_dim(value_acc, start, key_width, 0) + value_part, start, 0)
        return ((key_acc, value_acc), (attended.reshape(TOK_DEV, feature), query_grad.reshape(TOK_DEV, feature)))
    zeros_acc = jnp.zeros((pad_rows + TOKENS, feature), jnp.float32)
    (key_acc, value_acc), (attended, query_grad) = lax.scan(one_block, (zeros_acc, zeros_acc), jnp.arange(TOKENS // TOK_DEV, dtype=jnp.int32))
    return (attended.reshape(TOKENS, feature), query_grad.reshape(TOKENS, feature), key_acc[pad_rows:].astype(jnp.bfloat16), value_acc[pad_rows:].astype(jnp.bfloat16))
```

```python
import math

import jax
import jax.numpy as jnp
from jax import lax
from jax.experimental import pallas as pl
from jax.experimental.pallas import tpu as pltpu
from jax.sharding import PartitionSpec as P

HEADS = 16
REACH = 3
FWD_HEADS = 2
FAR_HEADS = 2
HIDE = -1e30


NT = (((1,), (1,)), ((), ()))
TN = (((0,), (0,)), ((), ()))
NN = (((1,), (0,)), ((), ()))


def dot(a, b, dims):
    return lax.dot_general(a, b, dims, preferred_element_type=jnp.float32)


def send(x, pairs):
    peers = lax.axis_size("seq")
    kept = [(i, j) for i, j in pairs if 0 <= j < peers]
    return lax.ppermute(x, "seq", kept)


def fwd_kernel(bias, q, g, k0, k1, k2, k3, v0, v1, v2, v3, o, dq, dk, dv, st):
    dim = q.shape[1] // FWD_HEADS
    inv = 1.0 / math.sqrt(dim)
    for h in range(FWD_HEADS):
        cols = slice(h * dim, (h + 1) * dim)
        qh, gh = q[:, cols], g[:, cols]
        ks = [r[:, cols] for r in (k0, k1, k2, k3)]
        vs = [r[:, cols] for r in (v0, v1, v2, v3)]
        s = [dot(k, qh, NT) * inv + bias[b] for b, k in enumerate(ks)]
        peak = jnp.max(s[0], 0, keepdims=True)
        for x in s[1:]:
            peak = jnp.maximum(peak, jnp.max(x, 0, keepdims=True))
        e = [jnp.exp(x - peak) for x in s]
        total = sum(jnp.sum(x, 0, keepdims=True) for x in e)
        recip = 1.0 / total
        w = [(x * recip).astype(jnp.bfloat16) for x in e]
        o[:, cols] = sum(dot(x, v, TN) for x, v in zip(w, vs)).astype(o.dtype)
        dp = [dot(v, gh, NT) for v in vs]
        delta = sum(
            jnp.sum(x.astype(jnp.float32) * y, 0, keepdims=True) for x, y in zip(w, dp)
        )
        ds = [
            (x.astype(jnp.float32) * (y - delta) * inv).astype(jnp.bfloat16)
            for x, y in zip(w, dp)
        ]
        dq[:, cols] = sum(dot(x, k, TN) for x, k in zip(ds, ks)).astype(dq.dtype)
        dk[:, cols] = dot(ds[0], qh, NN)
        dv[:, cols] = dot(w[0], gh, NN)
        st[h, 0:1, :] = peak + jnp.log(total)
        st[h, 1:2, :] = delta


def far_kernel(
    bias, k, v, dk0, dv0, q1, q2, q3, g1, g2, g3, s1, s2, s3, dk, dv
):
    dim = k.shape[1] // FAR_HEADS
    inv = 1.0 / math.sqrt(dim)
    for h in range(FAR_HEADS):
        cols = slice(h * dim, (h + 1) * dim)
        kh, vh = k[:, cols], v[:, cols]
        acc_k, acc_v = dk0[:, cols], dv0[:, cols]
        for b, (q, g, st) in enumerate(((q1, g1, s1), (q2, g2, s2), (q3, g3, s3))):
            qh, gh = q[:, cols], g[:, cols]
            s = dot(kh, qh, NT) * inv + bias[b]
            w = jnp.exp(s - st[h, 0:1, :]).astype(jnp.bfloat16)
            dp = dot(vh, gh, NT)
            ds = (w.astype(jnp.float32) * (dp - st[h, 1:2, :]) * inv).astype(jnp.bfloat16)
            acc_k = acc_k + dot(ds, qh, NN)
            acc_v = acc_v + dot(w, gh, NN)
        dk[:, cols] = acc_k.astype(dk.dtype)
        dv[:, cols] = acc_v.astype(dv.dtype)


def local(queries, keys, values, out_grad, segments):
    rows, feature = queries.shape
    dim = feature // HEADS
    peers = lax.axis_size("seq")
    index = lax.axis_index("seq")
    odd = index % 2
    every = range(peers)

    near_up = [(i, i + 1 if i % 2 == 0 else i + 3) for i in every]
    two_up = [(i, i + 2) for i in every]
    near_down = [(i, i - 1 if i % 2 == 1 else i - 3) for i in every]
    two_down = [(i, i - 2) for i in every]
    swap = [(i, i ^ 1) for i in every]

    key_two = send(keys, two_up)
    value_two = send(values, two_up)
    query_near = send(queries, near_down)
    grad_near = send(out_grad, near_down)
    key_near = send(keys, near_up)
    value_near = send(values, near_up)
    query_two = send(queries, two_down)
    grad_two = send(out_grad, two_down)
    key_swap = send(key_two, swap)
    value_swap = send(value_two, swap)
    query_swap = send(query_two, swap)
    grad_swap = send(grad_two, swap)

    seg_all = lax.all_gather(segments, "seq", tiled=True)
    edge = REACH * rows
    seg_pad = jnp.concatenate(
        [jnp.full((edge,), -1, jnp.int32), seg_all, jnp.full((edge,), -2, jnp.int32)]
    )

    def seg_at(offset):
        return lax.dynamic_slice_in_dim(seg_pad, (index + REACH + offset) * rows, rows)

    near, swapped = jnp.where(odd == 1, 1, 3), jnp.where(odd == 1, 3, 1)
    pos = jnp.arange(rows, dtype=jnp.int32)
    hide = jnp.float32(HIDE)
    key_segs = jnp.stack([segments, seg_at(-near), seg_at(-2), seg_at(-swapped)])
    seen = key_segs[:, :, None] == segments[None, None, :]
    causal = (pos[:, None] <= pos[None, :])[None] | (jnp.arange(REACH + 1) > 0)[:, None, None]
    bias = jnp.where(seen & causal, 0.0, hide)
    near_q, swapped_q = jnp.where(odd == 1, 3, 1), jnp.where(odd == 1, 1, 3)
    query_segs = jnp.stack([seg_at(near_q), seg_at(2), seg_at(swapped_q)])
    far_bias = jnp.where(query_segs[:, None, :] == segments[None, :, None], 0.0, hide)

    def wide(heads):
        return pl.BlockSpec((rows, heads * dim), lambda h: (0, h))

    def stat(heads):
        return pl.BlockSpec((heads, 2, rows), lambda h: (h, 0, 0))

    def whole(n):
        return pl.BlockSpec((n, rows, rows), lambda h: (0, 0, 0))

    half = jax.ShapeDtypeStruct((rows, feature), jnp.bfloat16)
    full = jax.ShapeDtypeStruct((rows, feature), jnp.float32)
    stats = jax.ShapeDtypeStruct((HEADS, 2, rows), jnp.float32)
    attended, query_grad, dk0, dv0, st = pl.pallas_call(
        fwd_kernel,
        grid=(HEADS // FWD_HEADS,),
        in_specs=[whole(REACH + 1)] + [wide(FWD_HEADS)] * 10,
        out_specs=[wide(FWD_HEADS)] * 4 + [stat(FWD_HEADS)],
        out_shape=[half, half, full, full, stats],
        name="fwd",
    )(
        bias, queries, out_grad, keys, key_near, key_two, key_swap,
        values, value_near, value_two, value_swap,
    )
    st_near = send(st, near_down)
    st_two = send(st, two_down)
    st_swap = send(st, [(i, i - 3 if i % 2 == 1 else i - 1) for i in every])
    key_grad, value_grad = pl.pallas_call(
        far_kernel,
        grid=(HEADS // FAR_HEADS,),
        in_specs=[whole(REACH)] + [wide(FAR_HEADS)] * 10 + [stat(FAR_HEADS)] * 3,
        out_specs=[wide(FAR_HEADS)] * 2,
        out_shape=[half, half],
        name="far",
    )(
        far_bias, keys, values, dk0, dv0, query_near, query_two, query_swap,
        grad_near, grad_two, grad_swap, st_near, st_two, st_swap,
    )
    return attended, query_grad, key_grad, value_grad


def solution(mesh):
    wide = P(("branch", "seq"), None)
    return jax.shard_map(
        local,
        mesh=mesh,
        in_specs=(wide, wide, wide, wide, P(("branch", "seq"))),
        out_specs=(wide, wide, wide, wide),
        check_vma=False,
    )
```

```python
import math
from functools import partial

import jax
import jax.numpy as jnp
from jax import lax
from jax.experimental import pallas as pl
from jax.experimental.pallas import tpu as pltpu
from jax.sharding import PartitionSpec as P

HEADS = 16
REACH = 3
FWD_HEADS = 2
FAR_HEADS = 2
HALVES = 2
TILE = 16
HIDE = -1e30


NT = (((1,), (1,)), ((), ()))
TN = (((0,), (0,)), ((), ()))
NN = (((1,), (0,)), ((), ()))


def dot(a, b, dims):
    return lax.dot_general(a, b, dims, preferred_element_type=jnp.float32)


def send(x, pairs):
    peers = lax.axis_size("seq")
    kept = [(i, j) for i, j in pairs if 0 <= j < peers]
    return lax.ppermute(x, "seq", kept)


def fwd_kernel(held, *refs):
    bias, q, g, k0, k1, k2, k3, v0, v1, v2, v3, o, dq, dk, dv, st = refs[held:]
    dim = q.shape[1] // FWD_HEADS
    inv = 1.0 / math.sqrt(dim)
    for h in range(FWD_HEADS):
        cols = slice(h * dim, (h + 1) * dim)
        qh, gh = q[:, cols], g[:, cols]
        ks = [r[:, cols] for r in (k0, k1, k2, k3)]
        vs = [r[:, cols] for r in (v0, v1, v2, v3)]
        s = [dot(k, qh, NT) * inv + bias[b] for b, k in enumerate(ks)]
        peak = jnp.max(s[0], 0, keepdims=True)
        for x in s[1:]:
            peak = jnp.maximum(peak, jnp.max(x, 0, keepdims=True))
        e = [jnp.exp(x - peak) for x in s]
        total = sum(jnp.sum(x, 0, keepdims=True) for x in e)
        recip = 1.0 / total
        w = [(x * recip).astype(jnp.bfloat16) for x in e]
        o[:, cols] = sum(dot(x, v, TN) for x, v in zip(w, vs)).astype(o.dtype)
        dp = [dot(v, gh, NT) for v in vs]
        delta = sum(
            jnp.sum(x.astype(jnp.float32) * y, 0, keepdims=True) for x, y in zip(w, dp)
        )
        ds = [
            (x.astype(jnp.float32) * (y - delta) * inv).astype(jnp.bfloat16)
            for x, y in zip(w, dp)
        ]
        dq[:, cols] = sum(dot(x, k, TN) for x, k in zip(ds, ks)).astype(dq.dtype)
        dk[:, cols] = dot(ds[0], qh, NN)
        dv[:, cols] = dot(w[0], gh, NN)
        st[h, 0:1, :] = peak + jnp.log(total)
        st[h, 1:2, :] = delta


def far_kernel(held, *refs):
    bias, k, v, dk0, dv0, q1, q2, q3, g1, g2, g3, s1, s2, s3, dk, dv = refs[held:]
    dim = k.shape[1] // FAR_HEADS
    inv = 1.0 / math.sqrt(dim)
    for h in range(FAR_HEADS):
        cols = slice(h * dim, (h + 1) * dim)
        kh, vh = k[:, cols], v[:, cols]
        acc_k, acc_v = dk0[:, cols], dv0[:, cols]
        for b, (q, g, st) in enumerate(((q1, g1, s1), (q2, g2, s2), (q3, g3, s3))):
            qh, gh = q[:, cols], g[:, cols]
            s = dot(kh, qh, NT) * inv + bias[b]
            w = jnp.exp(s - st[h, 0:1, :]).astype(jnp.bfloat16)
            dp = dot(vh, gh, NT)
            ds = (w.astype(jnp.float32) * (dp - st[h, 1:2, :]) * inv).astype(jnp.bfloat16)
            acc_k = acc_k + dot(ds, qh, NN)
            acc_v = acc_v + dot(w, gh, NN)
        dk[:, cols] = acc_k.astype(dk.dtype)
        dv[:, cols] = acc_v.astype(dv.dtype)


def pack_kernel(a, b, segs, *refs):
    outs, sems = refs[:HALVES], refs[HALVES]
    half = a.shape[1] // HALVES
    rows = a.shape[0]
    copies = [(segs, outs[0].at[pl.ds(rows, TILE), pl.ds(0, rows)])]
    for n, out in enumerate(outs):
        for m, src in enumerate((a, b)):
            dst = out.at[pl.ds(0, rows), pl.ds(m * half, half)]
            copies.append((src.at[:, pl.ds(n * half, half)], dst))
    copies = [pltpu.make_async_copy(x, y, sems.at[i]) for i, (x, y) in enumerate(copies)]
    for copy in copies:
        copy.start()
    for copy in copies:
        copy.wait()


def local(queries, keys, values, out_grad, segments):
    rows, feature = queries.shape
    dim = feature // HEADS
    half = feature // HALVES
    half_heads = HEADS // HALVES
    peers = lax.axis_size("seq")
    every = range(peers)

    near_up = [(i, i + 1 if i % 2 == 0 else i + 3) for i in every]
    two_up = [(i, i + 2) for i in every]
    near_down = [(i, i - 1 if i % 2 == 1 else i - 3) for i in every]
    two_down = [(i, i - 2) for i in every]
    swap_down = [(i, i - 3 if i % 2 == 1 else i - 1) for i in every]
    swap = [(i, i ^ 1) for i in every]

    own_seg = segments + 1
    seg_rows = jnp.broadcast_to(own_seg.astype(jnp.bfloat16)[None], (TILE, rows))

    def pack(a, b):
        wide = jax.ShapeDtypeStruct((rows, 2 * half), jnp.bfloat16)
        tall = jax.ShapeDtypeStruct((rows + TILE, 2 * half), jnp.bfloat16)
        spec = pl.BlockSpec(memory_space=pl.ANY)
        return pl.pallas_call(
            pack_kernel,
            in_specs=[spec] * 3,
            out_specs=[spec] * HALVES,
            out_shape=[tall] + [wide] * (HALVES - 1),
            scratch_shapes=[pltpu.SemaphoreType.DMA((2 * HALVES + 1,))],
        )(a, b, seg_rows)

    def seg_of(packed):
        return packed[rows, :rows].astype(jnp.int32)

    kv, qg = pack(keys, values), pack(queries, out_grad)
    kv_two, kv_near, qg_near, qg_two, kv_swap, qg_swap = [], [], [], [], [], []
    for n in range(HALVES):
        kv_two.append(send(kv[n], two_up))
        kv_near.append(send(kv[n], near_up))
    for n in range(HALVES):
        qg_near.append(send(qg[n], near_down))
        qg_two.append(send(qg[n], two_down))
    kv_swap.append(send(kv_two[0], swap))

    pos = jnp.arange(rows, dtype=jnp.int32)
    hide = jnp.float32(HIDE)
    key_segs = jnp.stack([own_seg] + [seg_of(x[0]) for x in (kv_near, kv_two, kv_swap)])
    seen = key_segs[:, :, None] == own_seg[None, None, :]
    causal = (pos[:, None] <= pos[None, :])[None] | (jnp.arange(REACH + 1) > 0)[:, None, None]
    bias = jnp.where(seen & causal, 0.0, hide)

    per_fwd, per_far = half // (FWD_HEADS * dim), half // (FAR_HEADS * dim)

    def wide(heads, first):
        return pl.BlockSpec((rows, heads * dim), lambda h: (0, h + first))

    def stat(heads):
        return pl.BlockSpec((heads, 2, rows), lambda h: (h, 0, 0))

    def whole(n):
        return pl.BlockSpec((n, rows, rows), lambda h: (0, 0, 0))

    anywhere = pl.BlockSpec(memory_space=pl.ANY)
    out = jax.ShapeDtypeStruct((rows, feature), jnp.bfloat16)
    part = jax.ShapeDtypeStruct((rows, half), jnp.float32)
    stats = jax.ShapeDtypeStruct((half_heads, 2, rows), jnp.float32)

    def run_fwd(n, before):
        at = n * per_fwd
        own, low, high = wide(FWD_HEADS, at), wide(FWD_HEADS, 0), wide(FWD_HEADS, per_fwd)
        got = (kv_near[n], kv_two[n], kv_swap[n])
        return pl.pallas_call(
            partial(fwd_kernel, len(before)),
            grid=(per_fwd,),
            in_specs=[anywhere] * len(before)
            + [whole(REACH + 1), own, own, own, low, low, low, own, high, high, high],
            out_specs=[own, own, low, low, stat(FWD_HEADS)],
            out_shape=[out, out, part, part, stats],
            input_output_aliases={i: i for i in range(len(before))},
        )(*before, bias, queries, out_grad, keys, *got, values, *got)

    def run_far(n, before, far_bias, dk0, dv0, st):
        at = n * per_far
        own, low, high = wide(FAR_HEADS, at), wide(FAR_HEADS, 0), wide(FAR_HEADS, per_far)
        got = (qg_near[n], qg_two[n], qg_swap[n])
        return pl.pallas_call(
            partial(far_kernel, len(before)),
            grid=(per_far,),
            in_specs=[anywhere] * len(before)
            + [whole(REACH), own, own, low, low, low, low, low, high, high, high]
            + [stat(FAR_HEADS)] * 3,
            out_specs=[own, own],
            out_shape=[out, out],
            input_output_aliases={i: i for i in range(len(before))},
        )(*before, far_bias, keys, values, dk0, dv0, *got, *got, *st)

    before, dk0, dv0, st = (), [], [], []
    for n in range(HALVES):
        if n > 0:
            mine, theirs, _ = lax.optimization_barrier((kv_two[n], kv_near[n], dk0[n - 1]))
            kv_two[n], kv_near[n] = mine, theirs
            kv_swap.append(send(mine, swap))
        *before, a, b, c = run_fwd(n, before)
        dk0.append(a)
        dv0.append(b)
        st.append([send(c, x) for x in (near_down, two_down, swap_down)])
    attended, query_grad = before

    *got, _ = lax.optimization_barrier((*qg_two, *qg_near, dk0[-1]))
    qg_two, qg_near = got[:HALVES], got[HALVES:]
    qg_swap = [send(x, swap) for x in qg_two]
    query_segs = jnp.stack([seg_of(x[0]) for x in (qg_near, qg_two, qg_swap)])
    far_bias = jnp.where(query_segs[:, None, :] == own_seg[None, :, None], 0.0, hide)
    before = ()
    for n in range(HALVES):
        before = run_far(n, before, far_bias, dk0[n], dv0[n], st[n])
    key_grad, value_grad = before
    return attended, query_grad, key_grad, value_grad


def solution(mesh):
    wide = P(("branch", "seq"), None)
    return jax.shard_map(
        local,
        mesh=mesh,
        in_specs=(wide, wide, wide, wide, P(("branch", "seq"))),
        out_specs=(wide, wide, wide, wide),
        check_vma=False,
    )
```

```python
import math
from functools import partial

import jax
import jax.numpy as jnp
from jax import lax
from jax.experimental import pallas as pl
from jax.sharding import PartitionSpec as P

HEADS = 16
REACH = 3
FWD_HEADS = 2
FAR_HEADS = 2
HALVES = 2
TILE = 16
HIDE = -1e30


NT = (((1,), (1,)), ((), ()))
TN = (((0,), (0,)), ((), ()))
NN = (((1,), (0,)), ((), ()))


def dot(a, b, dims):
    return lax.dot_general(a, b, dims, preferred_element_type=jnp.float32)


def send(x, pairs):
    peers = lax.axis_size("seq")
    kept = [(i, j) for i, j in pairs if 0 <= j < peers]
    return lax.ppermute(x, "seq", kept)


def fwd_kernel(held, *refs):
    bias, q, g, k0, k1, k2, k3, v0, v1, v2, v3, o, dq, dk, dv, st = refs[held:]
    dim = q.shape[1] // FWD_HEADS
    inv = 1.0 / math.sqrt(dim)
    for h in range(FWD_HEADS):
        cols = slice(h * dim, (h + 1) * dim)
        qh, gh = q[:, cols], g[:, cols]
        ks = [r[:, cols] for r in (k0, k1, k2, k3)]
        vs = [r[:, cols] for r in (v0, v1, v2, v3)]
        s = [dot(k, qh, NT) * inv + bias[b] for b, k in enumerate(ks)]
        peak = jnp.max(s[0], 0, keepdims=True)
        for x in s[1:]:
            peak = jnp.maximum(peak, jnp.max(x, 0, keepdims=True))
        e = [jnp.exp(x - peak) for x in s]
        total = sum(jnp.sum(x, 0, keepdims=True) for x in e)
        recip = 1.0 / total
        w = [(x * recip).astype(jnp.bfloat16) for x in e]
        o[:, cols] = sum(dot(x, v, TN) for x, v in zip(w, vs)).astype(o.dtype)
        dp = [dot(v, gh, NT) for v in vs]
        delta = sum(
            jnp.sum(x.astype(jnp.float32) * y, 0, keepdims=True) for x, y in zip(w, dp)
        )
        ds = [
            (x.astype(jnp.float32) * (y - delta) * inv).astype(jnp.bfloat16)
            for x, y in zip(w, dp)
        ]
        dq[:, cols] = sum(dot(x, k, TN) for x, k in zip(ds, ks)).astype(dq.dtype)
        dk[:, cols] = dot(ds[0], qh, NN)
        dv[:, cols] = dot(w[0], gh, NN)
        st[h, 0:1, :] = peak + jnp.log(total)
        st[h, 1:2, :] = delta


def far_kernel(held, *refs):
    bias, k, v, dk0, dv0, q1, q2, q3, g1, g2, g3, s1, s2, s3, dk, dv = refs[held:]
    dim = k.shape[1] // FAR_HEADS
    inv = 1.0 / math.sqrt(dim)
    for h in range(FAR_HEADS):
        cols = slice(h * dim, (h + 1) * dim)
        kh, vh = k[:, cols], v[:, cols]
        acc_k, acc_v = dk0[:, cols], dv0[:, cols]
        for b, (q, g, st) in enumerate(((q1, g1, s1), (q2, g2, s2), (q3, g3, s3))):
            qh, gh = q[:, cols], g[:, cols]
            s = dot(kh, qh, NT) * inv + bias[b]
            w = jnp.exp(s - st[h, 0:1, :]).astype(jnp.bfloat16)
            dp = dot(vh, gh, NT)
            ds = (w.astype(jnp.float32) * (dp - st[h, 1:2, :]) * inv).astype(jnp.bfloat16)
            acc_k = acc_k + dot(ds, qh, NN)
            acc_v = acc_v + dot(w, gh, NN)
        dk[:, cols] = acc_k.astype(dk.dtype)
        dv[:, cols] = acc_v.astype(dv.dtype)


def pack_kernel(a, b, segs, *outs):
    half, rows = a.shape[1] // HALVES, a.shape[0]
    for m, src in enumerate((a, b)):

        @pl.when(pl.program_id(0) == m)
        def _(src=src):
            for n, out in enumerate(outs):
                out[:rows, :] = src[:, n * half : (n + 1) * half]
            outs[0][rows:, :rows] = segs[...]
            outs[0][rows:, rows:] = jnp.zeros((TILE, half - rows), jnp.bfloat16)


def local(queries, keys, values, out_grad, segments):
    rows, feature = queries.shape
    dim = feature // HEADS
    half = feature // HALVES
    half_heads = HEADS // HALVES
    peers = lax.axis_size("seq")
    every = range(peers)

    near_up = [(i, i + 1 if i % 2 == 0 else i + 3) for i in every]
    two_up = [(i, i + 2) for i in every]
    near_down = [(i, i - 1 if i % 2 == 1 else i - 3) for i in every]
    two_down = [(i, i - 2) for i in every]
    swap_down = [(i, i - 3 if i % 2 == 1 else i - 1) for i in every]
    swap = [(i, i ^ 1) for i in every]

    own_seg = segments + 1
    seg_rows = jnp.broadcast_to(own_seg.astype(jnp.bfloat16)[None], (TILE, rows))

    def pack(a, b):
        wide = jax.ShapeDtypeStruct((rows, 2 * half), jnp.bfloat16)
        tall = jax.ShapeDtypeStruct((rows + TILE, 2 * half), jnp.bfloat16)
        full = pl.BlockSpec((rows, feature), lambda m: (0, 0))
        return pl.pallas_call(
            pack_kernel,
            grid=(2,),
            in_specs=[full, full, pl.BlockSpec((TILE, rows), lambda m: (0, 0))],
            out_specs=[pl.BlockSpec((rows + TILE, half), lambda m: (0, m))]
            + [pl.BlockSpec((rows, half), lambda m: (0, m))] * (HALVES - 1),
            out_shape=[tall] + [wide] * (HALVES - 1),
        )(a, b, seg_rows)

    def seg_of(packed):
        return packed[rows, :rows].astype(jnp.int32)

    kv, qg = pack(keys, values), pack(queries, out_grad)
    kv_two, kv_near, qg_near, qg_two, kv_swap, qg_swap = [], [], [], [], [], []
    for n in range(HALVES):
        kv_two.append(send(kv[n], two_up))
        kv_near.append(send(kv[n], near_up))
    for n in range(HALVES):
        qg_near.append(send(qg[n], near_down))
        qg_two.append(send(qg[n], two_down))
    kv_swap.append(send(kv_two[0], swap))

    pos = jnp.arange(rows, dtype=jnp.int32)
    hide = jnp.float32(HIDE)
    key_segs = jnp.stack([own_seg] + [seg_of(x[0]) for x in (kv_near, kv_two, kv_swap)])
    seen = key_segs[:, :, None] == own_seg[None, None, :]
    causal = (pos[:, None] <= pos[None, :])[None] | (jnp.arange(REACH + 1) > 0)[:, None, None]
    bias = jnp.where(seen & causal, 0.0, hide)

    per_fwd, per_far = half // (FWD_HEADS * dim), half // (FAR_HEADS * dim)

    def wide(heads, first):
        return pl.BlockSpec((rows, heads * dim), lambda h: (0, h + first))

    def stat(heads):
        return pl.BlockSpec((heads, 2, rows), lambda h: (h, 0, 0))

    def whole(n):
        return pl.BlockSpec((n, rows, rows), lambda h: (0, 0, 0))

    anywhere = pl.BlockSpec(memory_space=pl.ANY)
    out = jax.ShapeDtypeStruct((rows, feature), jnp.bfloat16)
    part = jax.ShapeDtypeStruct((rows, half), jnp.float32)
    stats = jax.ShapeDtypeStruct((half_heads, 2, rows), jnp.float32)

    def run_fwd(n, before):
        at = n * per_fwd
        own, low, high = wide(FWD_HEADS, at), wide(FWD_HEADS, 0), wide(FWD_HEADS, per_fwd)
        got = (kv_near[n], kv_two[n], kv_swap[n])
        return pl.pallas_call(
            partial(fwd_kernel, len(before)),
            grid=(per_fwd,),
            in_specs=[anywhere] * len(before)
            + [whole(REACH + 1), own, own, own, low, low, low, own, high, high, high],
            out_specs=[own, own, low, low, stat(FWD_HEADS)],
            out_shape=[out, out, part, part, stats],
            input_output_aliases={i: i for i in range(len(before))},
        )(*before, bias, queries, out_grad, keys, *got, values, *got)

    def run_far(n, before, far_bias, dk0, dv0, st):
        at = n * per_far
        own, low, high = wide(FAR_HEADS, at), wide(FAR_HEADS, 0), wide(FAR_HEADS, per_far)
        got = (qg_near[n], qg_two[n], qg_swap[n])
        return pl.pallas_call(
            partial(far_kernel, len(before)),
            grid=(per_far,),
            in_specs=[anywhere] * len(before)
            + [whole(REACH), own, own, low, low, low, low, low, high, high, high]
            + [stat(FAR_HEADS)] * 3,
            out_specs=[own, own],
            out_shape=[out, out],
            input_output_aliases={i: i for i in range(len(before))},
        )(*before, far_bias, keys, values, dk0, dv0, *got, *got, *st)

    before, dk0, dv0, st = (), [], [], []
    for n in range(HALVES):
        if n > 0:
            mine, theirs, _ = lax.optimization_barrier((kv_two[n], kv_near[n], dk0[n - 1]))
            kv_two[n], kv_near[n] = mine, theirs
            kv_swap.append(send(mine, swap))
        *before, a, b, c = run_fwd(n, before)
        dk0.append(a)
        dv0.append(b)
        ways = (near_down, two_down, swap_down)
        st.append([send(c, x) for x in ways])
    attended, query_grad = before

    def swap_qg(n, after):
        qg_two[n], qg_near[n], _ = lax.optimization_barrier((qg_two[n], qg_near[n], after))
        qg_swap.append(send(qg_two[n], swap))

    swap_qg(0, dk0[-1])
    query_segs = jnp.stack([seg_of(x[0]) for x in (qg_near, qg_two, qg_swap)])
    far_bias = jnp.where(query_segs[:, None, :] == own_seg[None, :, None], 0.0, hide)
    before = ()
    for n in range(HALVES):
        if n > 0:
            swap_qg(n, before[0])
        before = run_far(n, before, far_bias, dk0[n], dv0[n], st[n])
    key_grad, value_grad = before
    return attended, query_grad, key_grad, value_grad


def solution(mesh):
    wide = P(("branch", "seq"), None)
    return jax.shard_map(
        local,
        mesh=mesh,
        in_specs=(wide, wide, wide, wide, P(("branch", "seq"))),
        out_specs=(wide, wide, wide, wide),
        check_vma=False,
    )
```
